512 devices in a mesh: survey: 2 (over y), gz: 32 (over z), gy: 4 (over x), pat: 2 (over core).
Axes of the slice: x: 4, y: 2, z: 32, core: 2. Of those that a mesh axis runs over, the one named last changes fastest.
The devices are a block of a 4x16x32 slice.
Arguments:
- conductivity: float32 [256, 512, 512], P(('survey', 'gz'), 'gy'), parts along dimension 0, may hold values from 0.3 to 3
- receivers: int32 [4, 3, 64], P(('survey', 'pat')), parts along dimension 0, may hold values from 0 to 511, as said below
- observed: float32 [4, 64], P(('survey', 'pat')), parts along dimension 0, may hold values from -6 to 6
- potential: float32 [2, 256, 512, 512], P('pat', ('survey', 'gz'), 'gy'), parts along dimension 1, may hold values from -6 to 6
- adjoint_prev: float32 [2, 256, 512, 512], P('pat', ('survey', 'gz'), 'gy'), parts along dimension 1, may hold values from -0.046875 to 0.046875
Outputs:
- adjoint: float32 [2, 256, 512, 512], P('pat', ('survey', 'gz'), 'gy'), parts along dimension 1
- gradient: float32 [256, 512, 512], P(('survey', 'gz'), 'gy'), parts along dimension 0
The draws below stay inside these ranges and needn't reach their ends.
There are 2 independent parts, one for each index of `survey`. The reference program is written for one: setup_inputs(seed, part) draws one part's arguments, and reference() takes and returns one part's arrays. A program takes and returns all parts, laid end to end along the dimension named above; each array names one. Nothing has to cross between parts.
Inputs may be any that keep to these rules, and one draw needn't show every extreme that they name: receivers[p, 0, r], receivers[p, 1, r] and receivers[p, 2, r] are a z cell below 128, a y cell below 512 and an x cell below 512; several receivers may share a cell.
All inputs are finite; a program needn't handle non-finite values.
Results may differ from the reference program's by a relative error of at most 0.0003.
Values sent between devices are 32-bit elements; how exact they have to be, the bound alone decides.
No kernel may reach another device: no remote copies, remote signals or barrier semaphores. Data moves between devices by JAX's collectives and lax.ppermute only.
A program may use at most 64 MiB of HBM per device.

```python
import math
import jax
import jax.numpy as jnp
from jax import lax

NX = 512
RECV = 64
SWEEPS = 2
NZ = 128
NY = 512
PATTERNS = 2


def draw_receivers(key, part):
    key_z, key_y, key_x = jax.random.split(jax.random.fold_in(key, 11), 3)
    z_cell = jax.random.randint(key_z, (PATTERNS, 1, RECV), 0, NZ)
    y_cell = jax.random.randint(key_y, (PATTERNS, 1, RECV), 0, NY)
    x_cell = jax.random.randint(key_x, (PATTERNS, 1, RECV), 0, NX)
    return jnp.concatenate([z_cell, y_cell, x_cell], axis=1).astype(jnp.int32)


def block_scale(key, shape, cuts, smallest, largest):
    gain = 1.0
    for dim, blocks in cuts:
        draws = jax.random.uniform(jax.random.fold_in(jax.random.fold_in(key, 6), dim), (blocks,), jnp.float32, smallest / len(cuts), largest / len(cuts))
        gain = gain * jnp.repeat(jnp.exp(draws), shape[dim] // blocks).reshape((-1,) + (1,) * (len(shape) - 1 - dim))
    return gain


def normal_values(stream_key, shape, spread, bound, pieces=(), kind=jnp.bfloat16):
    gain = block_scale(stream_key, shape, pieces, -0.22, 0.18) if pieces else 1.0
    entries = jax.random.normal(stream_key, shape, jnp.float32) * spread * gain
    return jnp.minimum(jnp.maximum(entries, -bound), bound).astype(kind)


def setup_inputs(seed: int = 0, part: int = 0) -> dict:
    splits = jax.random.split(jax.random.key(seed), 6)
    part_splits = jax.random.split(jax.random.fold_in(splits[5], part), 6)
    conductivity = jnp.clip(jnp.exp(math.log(3.0) - 2.3025851 * jax.random.uniform(part_splits[0], (NZ, NY, NX), jnp.float32) ** block_scale(part_splits[0], (NZ, NY, NX), ((0, 32), (1, 4)), -0.2, 0.2)), 0.3, 3.0)
    receivers = draw_receivers(jax.random.fold_in(jax.random.fold_in(splits[5], part), 71), part)
    observed = normal_values(part_splits[2], (PATTERNS, RECV), 1.5, 6.0, ((0, 2),), jnp.float32)
    potential = normal_values(part_splits[3], (PATTERNS, NZ, NY, NX), 1.0, 6.0, ((0, 2), (1, 32), (2, 4)), jnp.float32)
    adjoint_prev = normal_values(part_splits[4], (PATTERNS, NZ, NY, NX), 0.003, 0.046875, ((0, 2), (1, 32), (2, 4)), jnp.float32)
    return {"conductivity": conductivity, "receivers": receivers, "observed": observed, "potential": potential, "adjoint_prev": adjoint_prev}


relax_weight = 0.8


def beside_cells(extended):
    widened = jnp.pad(extended, [(0, 0)] * (extended.ndim - 1) + [(1, 1)])
    centre = widened[..., 1:-1, 1:-1, 1:-1]
    others = [widened[..., 2:, 1:-1, 1:-1], widened[..., :-2, 1:-1, 1:-1],
              widened[..., 1:-1, 2:, 1:-1], widened[..., 1:-1, :-2, 1:-1],
              widened[..., 1:-1, 1:-1, 2:], widened[..., 1:-1, 1:-1, :-2]]
    return centre, others


def pad_rim(field):
    return jnp.pad(field, [(0, 0)] * (field.ndim - 3) + [(1, 1), (1, 1), (0, 0)])


def relax(cond_ext, adjoint_ext, source):
    cond_mid, cond_near = beside_cells(cond_ext)
    adj_mid, adj_near = beside_cells(adjoint_ext)
    diagonal = jnp.zeros_like(cond_mid)
    coupled = jnp.zeros_like(adj_mid)
    for cond_side, adj_side in zip(cond_near, adj_near):
        face_coef = 0.5 * (cond_mid + cond_side)
        diagonal = diagonal + face_coef
        coupled = coupled + face_coef * adj_side
    return adj_mid + relax_weight * (source - diagonal * adj_mid + coupled) / diagonal


def contribution(pot_ext, adj_ext):
    pot_mid, pot_near = beside_cells(pot_ext)
    adj_mid, adj_near = beside_cells(adj_ext)
    summed = jnp.zeros_like(adj_mid)
    for pot_side, adj_side in zip(pot_near, adj_near):
        summed = summed + (pot_mid - pot_side) * (adj_mid - adj_side)
    return -0.5 * jnp.sum(summed, axis=0)


def receiver_source(field, receivers, observed, z_start, y_start):
    z_count = field.shape[1]
    y_count = field.shape[2]
    z_local = receivers[:, 0, :] - z_start
    y_local = receivers[:, 1, :] - y_start
    x_local = receivers[:, 2, :]
    inside = (z_local >= 0) & (z_local < z_count) & (y_local >= 0) & (y_local < y_count)
    z_local = jnp.clip(z_local, 0, z_count - 1).astype(jnp.int32)
    y_local = jnp.clip(y_local, 0, y_count - 1).astype(jnp.int32)
    pattern_ids = jnp.broadcast_to(jnp.arange(field.shape[0], dtype=jnp.int32)[:, None], z_local.shape)
    values = jnp.where(inside, field[pattern_ids, z_local, y_local, x_local] - observed, jnp.zeros_like(observed))
    return jnp.zeros_like(field).at[pattern_ids, z_local, y_local, x_local].add(values)


def reference(conductivity, receivers, observed, potential, adjoint_prev):
    cond_ext = pad_rim(conductivity)

    def one_pattern(inputs):
        pot_one, adj_one, recv_one, obs_one = inputs
        pot_one = pot_one[None]
        source = receiver_source(pot_one, recv_one[None], obs_one[None], 0, 0)
        field = adj_one[None]
        for sweep_index in range(SWEEPS):
            field = relax(cond_ext, pad_rim(field), source)
        return field[0], contribution(pad_rim(pot_one), pad_rim(field))

    adjoint, terms = lax.map(one_pattern, (potential, adjoint_prev, receivers, observed))
    return adjoint, jnp.sum(terms, axis=0)
```

```python
import jax
import jax.numpy as jnp
from jax import lax
from jax.experimental import pallas as pl
from jax.experimental.pallas import tpu as pltpu
from jax.sharding import PartitionSpec as P


F32 = jnp.float32
VMEM = pl.BlockSpec(memory_space=pltpu.VMEM)
SMEM = pl.BlockSpec(memory_space=pltpu.SMEM)
HBM = pl.BlockSpec(memory_space=pltpu.HBM)
W = 3


def pack_kernel(
    rec_hbm, obs_hbm, cond, adj, pot,
    z_down, z_up, c_down, c_up, y_down, y_up, down_down, down_up, up_down, up_up,
    picked, field, rims, rec, obs, near, edge_sem, field_sem, plane_sem, list_sem,
):
    z_cells, y_cells, lanes = pot.shape
    count = obs.shape[1]
    lists = [
        pltpu.make_async_copy(rec_hbm, rec, list_sem.at[0]),
        pltpu.make_async_copy(obs_hbm, obs, list_sem.at[1]),
    ]
    for copy in lists:
        copy.start()
    z_first = lax.axis_index("gz") * z_cells
    y_first = lax.axis_index("gy") * y_cells
    end = y_cells - 8
    last = (W + 1) * y_cells
    edges = [
        pltpu.make_async_copy(x.at[:, pl.ds(first, 8), :], rims.at[i], edge_sem.at[i])
        for i, (x, first) in enumerate((x, first) for x in (cond, adj, pot) for first in (0, end))
    ]
    fields = [
        pltpu.make_async_copy(pot.at[k], field.at[k], field_sem.at[k]) for k in range(z_cells)
    ]
    moves = []
    for k in range(W):
        rows = pl.ds(k * y_cells, y_cells)
        top = z_cells - W + k
        moves += [(adj.at[top], z_up.at[rows]), (adj.at[k], z_down.at[rows])]
        moves += [(cond.at[top], c_up.at[k]), (cond.at[k], c_down.at[k])]
    rows = pl.ds(W * y_cells, y_cells)
    moves += [(pot.at[z_cells - 1], z_up.at[rows]), (pot.at[0], z_down.at[rows])]
    planes = [
        pltpu.make_async_copy(a, b, plane_sem.at[i]) for i, (a, b) in enumerate(moves)
    ]
    for copy in fields + edges + planes:
        copy.start()
    picked[...] = jnp.zeros_like(picked)
    lane = lax.broadcasted_iota(jnp.int32, (1, lanes), 1)

    for copy in lists:
        copy.wait()

    def listed(r, found):
        z = rec[0, 0, r] - z_first
        y = rec[1, 0, r] - y_first
        near[found] = r
        inside = (z >= 0) & (z < z_cells) & (y >= 0) & (y < y_cells)
        return found + inside.astype(jnp.int32)

    found = lax.fori_loop(0, count, listed, 0, unroll=8)
    for copy in fields:
        copy.wait()

    def one(n, carry):
        r = near[n]
        z = jnp.clip(rec[0, 0, r] - z_first, 0, z_cells - 1)
        y = jnp.clip(rec[1, 0, r] - y_first, 0, y_cells - 1)
        row = field[z, pl.ds(y, 1), :] - obs[0, r]
        picked[pl.ds(r, 1), :] = jnp.where(lane == rec[2, 0, r], row, 0.0)
        return carry

    lax.fori_loop(0, found, one, 0)
    column = jnp.sum(picked[...], axis=1, keepdims=True)
    eye = lax.broadcasted_iota(jnp.int32, (count, lanes), 0) == lax.broadcasted_iota(
        jnp.int32, (count, lanes), 1
    )
    values = jnp.sum(jnp.where(eye, column, 0.0), axis=0, keepdims=True)

    for copy in edges:
        copy.wait()
    for k in range(z_cells):
        y_down[k, 0:3, :] = rims[0, k, 0:3, :]
        y_down[k, 3:6, :] = rims[2, k, 0:3, :]
        y_down[k, 6:7, :] = rims[4, k, 0:1, :]
        y_down[k, 7:8, :] = values
        y_up[k, 0:3, :] = rims[1, k, 5:8, :]
        y_up[k, 3:6, :] = rims[3, k, 5:8, :]
        y_up[k, 6:7, :] = rims[5, k, 7:8, :]
        y_up[k, 7:8, :] = values
    for k in range(W):
        top = z_cells - W + k
        down_down[k] = y_down[k]
        down_up[k] = y_up[k]
        up_down[k] = y_down[top]
        up_up[k] = y_up[top]
    z_down[last : last + 8, :] = jnp.broadcast_to(values, (8, lanes))
    z_up[last : last + 8, :] = jnp.broadcast_to(values, (8, lanes))
    for copy in planes:
        copy.wait()


def rim_rows(sub, low, high, first, depth):
    below = jnp.where(sub >= 8 - depth, pltpu.roll(low, (8 - depth - first) % 8, 0), 0.0)
    above = jnp.where(sub < depth, pltpu.roll(high, (8 - first) % 8, 0) if first else high, 0.0)
    return below, above


def piece(ref, k, j, chunks):
    return ref[k, pl.ds(8 * j, 8), :] if 0 <= j < chunks + 2 else jnp.zeros((8, ref.shape[2]), F32)


def weight_kernel(
    cond, c_lo, c_hi, d_lo, d_hi, y_lo, y_hi, lo_lo, lo_hi, hi_lo, hi_hi,
    we, tx, ty, tz, ce,
):
    z_cells, y_cells, lanes = cond.shape
    chunks = y_cells // 8
    planes = z_cells + 2 * W
    z_first = lax.axis_index("gz") * z_cells
    y_first = lax.axis_index("gy") * y_cells
    z_total = lax.axis_size("gz") * z_cells
    y_total = lax.axis_size("gy") * y_cells
    sub = lax.broadcasted_iota(jnp.int32, (8, lanes), 0)
    lane = lax.broadcasted_iota(jnp.int32, (8, lanes), 1)
    right = lanes - 1
    body = pl.ds(8, y_cells)
    end = pl.ds(y_cells + 8, 8)
    for k in range(z_cells):
        ce[W + k, body, :] = cond[k]
    for k in range(planes):
        if k < W:
            low, high = lo_lo[k], lo_hi[k]
        elif k < W + z_cells:
            low, high = y_lo[k - W], y_hi[k - W]
        else:
            low, high = hi_lo[k - W - z_cells], hi_hi[k - W - z_cells]
        ce[k, 0:8, :], ce[k, end, :] = rim_rows(sub, low, high, 0, 3)
    direct = lax.axis_index("pat") == 1

    @pl.when(direct)
    def _():
        for k in range(W):
            ce[k, body, :] = c_lo[k]
            ce[W + z_cells + k, body, :] = c_hi[k]

    @pl.when(jnp.logical_not(direct))
    def _():
        for k in range(W):
            ce[k, body, :] = d_lo[k]
            ce[W + z_cells + k, body, :] = d_hi[k]

    for j in range(chunks + 2):
        at = pl.ds(8 * j, 8)
        tz[0, at, :] = ce[0, at, :] + ce[1, at, :]

    def plane(k, carry):
        z = z_first + k - W
        z_inside = (z >= 0) & (z < z_total)
        c_up = pltpu.roll(piece(ce, k, 0, chunks), 7, 0)
        face_before = jnp.zeros((8, lanes), F32)
        for j in range(chunks + 2):
            at = pl.ds(8 * j, 8)
            c = piece(ce, k, j, chunks)
            c_next = pltpu.roll(piece(ce, k, j + 1, chunks), 7, 0)
            face_y = c + jnp.where(sub == 7, c_next, c_up)
            face_y_down = pltpu.roll(face_y, 1, 0)
            face_x = c + pltpu.roll(c, right, 1)
            face_z = c + ce[k + 1, at, :]
            total = face_y + jnp.where(sub == 0, face_before, face_y_down)
            total += jnp.where(lane == right, c, face_x)
            total += jnp.where(lane == 0, c, pltpu.roll(face_x, 1, 1))
            total += face_z + tz[k - 1, at, :]
            y = sub + (y_first + 8 * j - 8)
            known = z_inside & (y >= 0) & (y < y_total)
            if j == 0:
                known = known & (sub >= 5)
            if j == chunks + 1:
                known = known & (sub < 3)
            we[k, at, :] = jnp.where(known, 0.8 / jnp.where(known, total, 1.0), 0.0)
            tx[k, at, :] = jnp.where(lane == right, 0.0, face_x)
            ty[k, at, :] = face_y
            tz[k, at, :] = face_z
            c_up, face_before = c_next, face_y_down
        return carry

    lax.fori_loop(1, planes - 1, plane, 0)


def sweep_kernel(
    rec_hbm, adj, we, tx, ty, tz, z_lo, z_hi, y_lo, y_hi, lo_lo, lo_hi, hi_lo, hi_hi, own,
    ae, be, vals, rec, near, list_sem,
):
    z_cells, y_cells, lanes = adj.shape
    count = vals.shape[0]
    chunks = y_cells // 8
    planes = z_cells + 2 * W
    z_first = lax.axis_index("gz") * z_cells
    y_first = lax.axis_index("gy") * y_cells
    sub = lax.broadcasted_iota(jnp.int32, (8, lanes), 0)
    lane = lax.broadcasted_iota(jnp.int32, (1, lanes), 1)
    right = lanes - 1
    body = pl.ds(8, y_cells)
    end = pl.ds(y_cells + 8, 8)
    listing = pltpu.make_async_copy(rec_hbm, rec, list_sem)
    listing.start()
    for k in range(planes):
        if k < W:
            low, high = lo_lo[k], lo_hi[k]
            ae[k, body, :] = z_lo[k * y_cells : (k + 1) * y_cells, :]
        elif k < W + z_cells:
            low, high = y_lo[k - W], y_hi[k - W]
            ae[k, body, :] = adj[k - W]
        else:
            n = k - W - z_cells
            low, high = hi_lo[n], hi_hi[n]
            ae[k, body, :] = z_hi[n * y_cells : (n + 1) * y_cells, :]
        ae[k, 0:8, :], ae[k, end, :] = rim_rows(sub, low, high, 3, 3)

    last = (W + 1) * y_cells
    values = own[0, 7:8, :] + z_lo[last : last + 1, :] + z_hi[last : last + 1, :]
    for side in (y_lo, y_hi, lo_lo, lo_hi, hi_lo, hi_hi):
        values += side[0, 7:8, :]
    eye = lax.broadcasted_iota(jnp.int32, (count, lanes), 0) == lax.broadcasted_iota(
        jnp.int32, (count, lanes), 1
    )
    vals[...] = jnp.broadcast_to(
        jnp.sum(jnp.where(eye, values, 0.0), axis=1, keepdims=True), (count, lanes)
    )
    listing.wait()

    def listed(r, found):
        k = rec[0, 0, r] - z_first + W
        j = rec[1, 0, r] - y_first + 8
        near[found] = r
        inside = (k >= 1) & (k < planes - 1) & (j >= 6) & (j < y_cells + 10)
        return found + inside.astype(jnp.int32)

    found = lax.fori_loop(0, count, listed, 0, unroll=8)

    def sweep(source, target, start, stop):
        def plane(k, carry):
            f_up = pltpu.roll(piece(source, k, 0, chunks), 7, 0)
            flux_before = jnp.zeros((8, lanes), F32)
            for j in range(chunks + 2):
                at = pl.ds(8 * j, 8)
                f = piece(source, k, j, chunks)
                f_next = pltpu.roll(piece(source, k, j + 1, chunks), 7, 0)
                face_x, face_y = tx[k, at, :], ty[k, at, :]
                flux_down = pltpu.roll(face_y * f, 1, 0)
                total = face_y * jnp.where(sub == 7, f_next, f_up)
                total += jnp.where(sub == 0, flux_before, flux_down)
                total += face_x * pltpu.roll(f, right, 1) + pltpu.roll(face_x * f, 1, 1)
                total += tz[k, at, :] * source[k + 1, at, :] + tz[k - 1, at, :] * source[k - 1, at, :]
                target[k, at, :] = 0.2 * f + we[k, at, :] * total
                f_up, flux_before = f_next, flux_down
            return carry

        lax.fori_loop(start, stop, plane, 0)

        def one(n, carry):
            r = near[n]
            k = rec[0, 0, r] - z_first + W
            at = pl.ds(jnp.clip(rec[1, 0, r] - y_first + 8, 6, y_cells + 9), 1)

            @pl.when((k >= start) & (k < stop))
            def _():
                kc = jnp.clip(k, start, stop - 1)
                add = 2.0 * we[kc, at, :] * vals[pl.ds(r, 1), :]
                target[kc, at, :] = target[kc, at, :] + jnp.where(lane == rec[2, 0, r], add, 0.0)

            return carry

        lax.fori_loop(0, found, one, 0)

    sweep(ae, be, 1, planes - 1)
    sweep(be, ae, 2, planes - 2)


def gradient_kernel(pot, ae, z_lo, z_hi, y_lo, y_hi, grad, adj_out, ve, out_sem):
    z_cells, y_cells, lanes = pot.shape
    chunks = y_cells // 8
    sub = lax.broadcasted_iota(jnp.int32, (8, lanes), 0)
    lane = lax.broadcasted_iota(jnp.int32, (8, lanes), 1)
    right = lanes - 1
    body = pl.ds(8, y_cells)
    end = pl.ds(y_cells + 8, 8)
    stores = [
        pltpu.make_async_copy(ae.at[W + k, body], adj_out.at[k], out_sem.at[k])
        for k in range(z_cells)
    ]
    for copy in stores:
        copy.start()
    plane_rows = slice(W * y_cells, (W + 1) * y_cells)
    ve[0, body, :] = z_lo[plane_rows, :]
    ve[z_cells + 1, body, :] = z_hi[plane_rows, :]
    for k in range(z_cells):
        ve[1 + k, body, :] = pot[k]
        ve[1 + k, 0:8, :], ve[1 + k, end, :] = rim_rows(sub, y_lo[k], y_hi[k], 6, 1)

    def plane(n, carry):
        k, q = n + W, n + 1

        def up(ref, m, j):
            return pltpu.roll(piece(ref, m, j, chunks), 7, 0)

        a, v = piece(ae, k, 0, chunks), piece(ve, q, 0, chunks)
        a_up, v_up = up(ae, k, 1), up(ve, q, 1)
        term_before = pltpu.roll(
            (v - jnp.where(sub == 7, v_up, v)) * (a - jnp.where(sub == 7, a_up, a)), 1, 0
        )
        for j in range(1, chunks + 1):
            at = pl.ds(8 * j, 8)
            a, v = piece(ae, k, j, chunks), piece(ve, q, j, chunks)
            a_next, v_next = up(ae, k, j + 1), up(ve, q, j + 1)
            term = (v - jnp.where(sub == 7, v_next, v_up)) * (a - jnp.where(sub == 7, a_next, a_up))
            term_down = pltpu.roll(term, 1, 0)
            total = term + jnp.where(sub == 0, term_before, term_down)
            term = (v - jnp.where(lane == right, 0.0, pltpu.roll(v, right, 1))) * (
                a - jnp.where(lane == right, 0.0, pltpu.roll(a, right, 1))
            )
            total += term + jnp.where(lane == 0, v * a, pltpu.roll(term, 1, 1))
            total += (v - ve[q - 1, at, :]) * (a - ae[k - 1, at, :])
            total += (v - ve[q + 1, at, :]) * (a - ae[k + 1, at, :])
            grad[n, pl.ds(8 * (j - 1), 8), :] = -0.5 * total
            term_before, a_up, v_up = term_down, a_next, v_next
        return carry

    lax.fori_loop(0, z_cells, plane, 0)
    for copy in stores:
        copy.wait()


def shifts(devices, step):
    return [(i, i + step) for i in range(devices) if 0 <= i + step < devices]


def both_ways(up, down, axis):
    devices = lax.axis_size(axis)
    return (
        lax.ppermute(up, axis, shifts(devices, 1)), lax.ppermute(down, axis, shifts(devices, -1))
    )


def step(conductivity, receivers, observed, potential, adjoint_prev):
    cond, pot, adj = conductivity, potential[0], adjoint_prev[0]
    z_cells, y_cells, lanes = cond.shape
    count = observed.shape[1]
    shape = jax.ShapeDtypeStruct

    block = shape((z_cells, y_cells, lanes), F32)
    edge = shape((z_cells, 8, lanes), F32)
    side = shape(((W + 1) * y_cells + 8, lanes), F32)
    thick = shape((W, y_cells, lanes), F32)
    corner = shape((W, 8, lanes), F32)
    rec = receivers.transpose(1, 0, 2)
    rec, obs, cond, adj, pot = (
        pltpu.with_memory_space_constraint(x, pltpu.HBM) for x in (rec, observed, cond, adj, pot)
    )
    z_down, z_up, c_down, c_up, y_down, y_up, dd, du, ud, uu = pl.pallas_call(
        pack_kernel,
        out_shape=(side, side, thick, thick, edge, edge) + (corner,) * 4,
        in_specs=[HBM] * 5,
        out_specs=(VMEM,) * 10,
        scratch_shapes=[
            pltpu.VMEM((count, lanes), F32),
            pltpu.VMEM((z_cells, y_cells, lanes), F32),
            pltpu.VMEM((6, z_cells, 8, lanes), F32),
            pltpu.SMEM((3, 1, count), jnp.int32),
            pltpu.SMEM((1, count), F32),
            pltpu.SMEM((count,), jnp.int32),
            pltpu.SemaphoreType.DMA((6,)),
            pltpu.SemaphoreType.DMA((z_cells,)),
            pltpu.SemaphoreType.DMA((4 * W + 2,)),
            pltpu.SemaphoreType.DMA((2,)),
        ],
        compiler_params=pltpu.CompilerParams(vmem_limit_bytes=16 * 1024 * 1024),
        name="pack",
    )(rec, obs, cond, adj, pot)

    deep = lax.axis_size("gz")
    c_lo = lax.ppermute(c_up, ("gz", "pat"), [(2 * i + 1, 2 * i + 3) for i in range(deep - 1)])
    c_hi = lax.ppermute(c_down, ("gz", "pat"), [(2 * i + 3, 2 * i + 1) for i in range(deep - 1)])
    z_lo, z_hi = both_ways(z_up, z_down, "gz")
    y_lo, y_hi = both_ways(y_up, y_down, "gy")
    wide = lax.axis_size("gy")

    def diagonal(x, up_z, up_y):
        pairs = [
            (i * wide + j, (i + up_z) * wide + j + up_y)
            for i in range(deep) if 0 <= i + up_z < deep
            for j in range(wide) if 0 <= j + up_y < wide
        ]
        return lax.ppermute(x, ("gz", "gy"), pairs)

    lo_lo = diagonal(uu, 1, 1)
    lo_hi = diagonal(ud, 1, -1)
    hi_lo = diagonal(du, -1, 1)
    hi_hi = diagonal(dd, -1, -1)
    d_lo = lax.ppermute(c_lo, "pat", [(1, 0)])
    d_hi = lax.ppermute(c_hi, "pat", [(1, 0)])

    full = (z_cells + 2 * W, y_cells + 16, lanes)
    ext = shape(full, F32)
    we, tx, ty, tz = pl.pallas_call(
        weight_kernel,
        out_shape=(ext,) * 4,
        in_specs=[VMEM] * 11,
        out_specs=(VMEM,) * 4,
        scratch_shapes=[pltpu.VMEM(full, F32)],
        compiler_params=pltpu.CompilerParams(vmem_limit_bytes=20 * 1024 * 1024),
        name="weights",
    )(conductivity, c_lo, c_hi, d_lo, d_hi, y_lo, y_hi, lo_lo, lo_hi, hi_lo, hi_hi)
    relaxed = pl.pallas_call(
        sweep_kernel,
        out_shape=ext,
        in_specs=[HBM] + [VMEM] * 14,
        out_specs=VMEM,
        scratch_shapes=[
            pltpu.VMEM(full, F32),
            pltpu.VMEM((count, lanes), F32),
            pltpu.SMEM((3, 1, count), jnp.int32),
            pltpu.SMEM((count,), jnp.int32),
            pltpu.SemaphoreType.DMA,
        ],
        compiler_params=pltpu.CompilerParams(vmem_limit_bytes=20 * 1024 * 1024),
        name="sweeps",
    )(rec, adjoint_prev[0], we, tx, ty, tz, z_lo, z_hi, y_lo, y_hi, lo_lo, lo_hi, hi_lo, hi_hi, y_up)
    part, adjoint = pl.pallas_call(
        gradient_kernel,
        out_shape=(block, block),
        in_specs=[VMEM] * 6,
        out_specs=(VMEM, HBM),
        scratch_shapes=[
            pltpu.VMEM((z_cells + 2, y_cells + 16, lanes), F32),
            pltpu.SemaphoreType.DMA((z_cells,)),
        ],
        compiler_params=pltpu.CompilerParams(vmem_limit_bytes=16 * 1024 * 1024),
        name="gradient",
    )(potential[0], relaxed, z_lo, z_hi, y_lo, y_hi)
    other = lax.ppermute(part, "pat", [(0, 1), (1, 0)])
    return adjoint[None], part + other


def solution(mesh):
    return jax.shard_map(
        step,
        mesh=mesh,
        in_specs=(
            P(("survey", "gz"), "gy", None),
            P(("survey", "pat"), None, None),
            P(("survey", "pat"), None),
            P("pat", ("survey", "gz"), "gy", None),
            P("pat", ("survey", "gz"), "gy", None),
        ),
        out_specs=(P("pat", ("survey", "gz"), "gy", None), P(("survey", "gz"), "gy", None)),
        check_vma=False,
    )
```

```python
import jax
import jax.numpy as jnp
from jax import lax
from jax.experimental import pallas as pl
from jax.experimental.pallas import tpu as pltpu
from jax.sharding import PartitionSpec as P


F32 = jnp.float32
VMEM = pl.BlockSpec(memory_space=pltpu.VMEM)
SMEM = pl.BlockSpec(memory_space=pltpu.SMEM)
HBM = pl.BlockSpec(memory_space=pltpu.HBM)
W = 3


def within(i, count):
    return i.astype(jnp.uint32) < jnp.uint32(count)


def pack_kernel(
    rec_hbm, obs_hbm, cond, adj, pot,
    z_down, z_up, c_down, c_up, y_down, y_up, down_down, down_up, up_down, up_up,
    picked, field, rims, rec, obs, near, edge_sem, field_sem, plane_sem,
    thick_sem, list_sem,
):
    z_cells, y_cells, lanes = pot.shape
    count = obs.shape[1]
    lists = [
        pltpu.make_async_copy(rec_hbm, rec, list_sem.at[0]),
        pltpu.make_async_copy(obs_hbm, obs, list_sem.at[1]),
    ]
    for copy in lists:
        copy.start()
    z_first = lax.axis_index("gz") * z_cells
    y_first = lax.axis_index("gy") * y_cells
    end = y_cells - 8
    last = (W + 1) * y_cells
    edges = [
        pltpu.make_async_copy(x.at[:, pl.ds(first, 8), :], rims.at[i], edge_sem.at[i])
        for i, (x, first) in enumerate((x, first) for x in (cond, adj, pot) for first in (0, end))
    ]
    fields = [
        pltpu.make_async_copy(pot.at[k], field.at[k], field_sem.at[k]) for k in range(z_cells)
    ]
    moves, shared = [], []
    for k in range(W):
        rows = pl.ds(k * y_cells, y_cells)
        top = z_cells - W + k
        moves += [(adj.at[top], z_up.at[rows]), (adj.at[k], z_down.at[rows])]
        shared += [(cond.at[top], c_up.at[k]), (cond.at[k], c_down.at[k])]
    rows = pl.ds(W * y_cells, y_cells)
    moves += [(pot.at[z_cells - 1], z_up.at[rows]), (pot.at[0], z_down.at[rows])]
    planes = [
        pltpu.make_async_copy(a, b, plane_sem.at[i]) for i, (a, b) in enumerate(moves)
    ]
    thick = [
        pltpu.make_async_copy(a, b, thick_sem.at[i]) for i, (a, b) in enumerate(shared)
    ]
    direct = lax.axis_index("pat") == 1
    for copy in fields + edges + planes:
        copy.start()

    @pl.when(direct)
    def _():
        for copy in thick:
            copy.start()

    picked[...] = jnp.zeros_like(picked)
    lane = lax.broadcasted_iota(jnp.int32, (1, lanes), 1)

    for copy in lists:
        copy.wait()

    def listed(r, found):
        z = rec[0, 0, r] - z_first
        y = rec[1, 0, r] - y_first
        near[found] = r
        return found + jnp.where(within(z, z_cells) & within(y, y_cells), 1, 0)

    found = lax.fori_loop(0, count, listed, 0, unroll=8)
    for copy in fields:
        copy.wait()

    def one(n, carry):
        r = near[n]
        z = jnp.clip(rec[0, 0, r] - z_first, 0, z_cells - 1)
        y = jnp.clip(rec[1, 0, r] - y_first, 0, y_cells - 1)
        row = field[z, pl.ds(y, 1), :] - obs[0, r]
        picked[pl.ds(r, 1), :] = jnp.where(lane == rec[2, 0, r], row, 0.0)
        return carry

    lax.fori_loop(0, found, one, 0)
    column = jnp.sum(picked[...], axis=1, keepdims=True)
    eye = lax.broadcasted_iota(jnp.int32, (count, lanes), 0) == lax.broadcasted_iota(
        jnp.int32, (count, lanes), 1
    )
    values = jnp.sum(jnp.where(eye, column, 0.0), axis=0, keepdims=True)

    for copy in edges:
        copy.wait()
    for k in range(z_cells):
        y_down[k, 0:3, :] = rims[0, k, 0:3, :]
        y_down[k, 3:6, :] = rims[2, k, 0:3, :]
        y_down[k, 6:7, :] = rims[4, k, 0:1, :]
        y_down[k, 7:8, :] = values
        y_up[k, 0:3, :] = rims[1, k, 5:8, :]
        y_up[k, 3:6, :] = rims[3, k, 5:8, :]
        y_up[k, 6:7, :] = rims[5, k, 7:8, :]
        y_up[k, 7:8, :] = values
    for k in range(W):
        top = z_cells - W + k
        down_down[k] = y_down[k]
        down_up[k] = y_up[k]
        up_down[k] = y_down[top]
        up_up[k] = y_up[top]
    z_down[last : last + 8, :] = jnp.broadcast_to(values, (8, lanes))
    z_up[last : last + 8, :] = jnp.broadcast_to(values, (8, lanes))
    for copy in planes:
        copy.wait()

    @pl.when(direct)
    def _():
        for copy in thick:
            copy.wait()


def rim_rows(sub, low, high, first, depth):
    below = jnp.where(sub >= 8 - depth, pltpu.roll(low, (8 - depth - first) % 8, 0), 0.0)
    above = jnp.where(sub < depth, pltpu.roll(high, (8 - first) % 8, 0) if first else high, 0.0)
    return below, above


def piece(ref, k, j, chunks):
    return ref[k, pl.ds(8 * j, 8), :] if 0 <= j < chunks + 2 else jnp.zeros((8, ref.shape[2]), F32)


def join_kernel(low, high, both):
    @pl.when(lax.axis_index("pat") == 1)
    def _():
        both[0:W] = low[...]
        both[W : 2 * W] = high[...]


def weight_kernel(
    cond, both, given, y_lo, y_hi, lo_lo, lo_hi, hi_lo, hi_hi,
    we, tx, ty, tz, ce,
):
    z_cells, y_cells, lanes = cond.shape
    chunks = y_cells // 8
    planes = z_cells + 2 * W
    z_first = lax.axis_index("gz") * z_cells
    y_first = lax.axis_index("gy") * y_cells
    z_total = lax.axis_size("gz") * z_cells
    y_total = lax.axis_size("gy") * y_cells
    sub = lax.broadcasted_iota(jnp.int32, (8, lanes), 0)
    lane = lax.broadcasted_iota(jnp.int32, (8, lanes), 1)
    right = lanes - 1
    body = pl.ds(8, y_cells)
    end = pl.ds(y_cells + 8, 8)
    for k in range(z_cells):
        ce[W + k, body, :] = cond[k]
    for k in range(planes):
        if k < W:
            low, high = lo_lo[k], lo_hi[k]
        elif k < W + z_cells:
            low, high = y_lo[k - W], y_hi[k - W]
        else:
            low, high = hi_lo[k - W - z_cells], hi_hi[k - W - z_cells]
        ce[k, 0:8, :], ce[k, end, :] = rim_rows(sub, low, high, 0, 3)
    direct = lax.axis_index("pat") == 1

    @pl.when(direct)
    def _():
        for k in range(W):
            ce[k, body, :] = both[k]
            ce[W + z_cells + k, body, :] = both[W + k]

    @pl.when(jnp.logical_not(direct))
    def _():
        for k in range(W):
            ce[k, body, :] = given[k]
            ce[W + z_cells + k, body, :] = given[W + k]

    for j in range(chunks + 2):
        at = pl.ds(8 * j, 8)
        tz[0, at, :] = ce[0, at, :] + ce[1, at, :]

    def plane(k, carry):
        z = z_first + k - W
        z_inside = (z >= 0) & (z < z_total)
        scale = jnp.where(z_inside, 0.8, 0.0)
        spare = jnp.where(z_inside, 0.0, 1.0)
        c = piece(ce, k, 0, chunks)
        c_up = pltpu.roll(c, 7, 0)
        face_before = jnp.zeros((8, lanes), F32)
        for j in range(chunks + 2):
            at = pl.ds(8 * j, 8)
            after = piece(ce, k, j + 1, chunks)
            c_next = pltpu.roll(after, 7, 0)
            face_y = c + jnp.where(sub == 7, c_next, c_up)
            face_y_down = pltpu.roll(face_y, 1, 0)
            face_x = c + pltpu.roll(c, right, 1)
            face_z = c + ce[k + 1, at, :]
            total = face_y + jnp.where(sub == 0, face_before, face_y_down)
            total += jnp.where(lane == right, c, face_x)
            total += jnp.where(lane == 0, c, pltpu.roll(face_x, 1, 1))
            total += face_z + tz[k - 1, at, :]
            if 0 < j < chunks + 1:
                we[k, at, :] = scale / (total + spare)
            else:
                y = sub + (y_first + 8 * j - 8)
                known = z_inside & (y >= 0) & (y < y_total)
                known = known & ((sub >= 5) if j == 0 else (sub < 3))
                we[k, at, :] = jnp.where(known, 0.8 / jnp.where(known, total, 1.0), 0.0)
            tx[k, at, :] = jnp.where(lane == right, 0.0, face_x)
            ty[k, at, :] = face_y
            tz[k, at, :] = face_z
            c, c_up, face_before = after, c_next, face_y_down
        return carry

    lax.fori_loop(1, planes - 1, plane, 0)


def sweep_kernel(
    rec_hbm, adj, we, tx, ty, tz, z_lo, z_hi, y_lo, y_hi, lo_lo, lo_hi, hi_lo, hi_hi, own,
    ae, be, vals, rec, near, list_sem,
):
    z_cells, y_cells, lanes = adj.shape
    count = vals.shape[0]
    chunks = y_cells // 8
    planes = z_cells + 2 * W
    z_first = lax.axis_index("gz") * z_cells
    y_first = lax.axis_index("gy") * y_cells
    sub = lax.broadcasted_iota(jnp.int32, (8, lanes), 0)
    lane = lax.broadcasted_iota(jnp.int32, (1, lanes), 1)
    right = lanes - 1
    body = pl.ds(8, y_cells)
    end = pl.ds(y_cells + 8, 8)
    listing = pltpu.make_async_copy(rec_hbm, rec, list_sem)
    listing.start()
    for k in range(planes):
        if k < W:
            low, high = lo_lo[k], lo_hi[k]
            ae[k, body, :] = z_lo[k * y_cells : (k + 1) * y_cells, :]
        elif k < W + z_cells:
            low, high = y_lo[k - W], y_hi[k - W]
            ae[k, body, :] = adj[k - W]
        else:
            n = k - W - z_cells
            low, high = hi_lo[n], hi_hi[n]
            ae[k, body, :] = z_hi[n * y_cells : (n + 1) * y_cells, :]
        ae[k, 0:8, :], ae[k, end, :] = rim_rows(sub, low, high, 3, 3)

    def sweep(source, target, start, stop):
        def plane(k, carry):
            f = piece(source, k, 0, chunks)
            f_up = pltpu.roll(f, 7, 0)
            flux_before = jnp.zeros((8, lanes), F32)
            for j in range(chunks + 2):
                at = pl.ds(8 * j, 8)
                after = piece(source, k, j + 1, chunks)
                f_next = pltpu.roll(after, 7, 0)
                face_x, face_y = tx[k, at, :], ty[k, at, :]
                flux_down = pltpu.roll(face_y * f, 1, 0)
                total = face_y * jnp.where(sub == 7, f_next, f_up)
                total += jnp.where(sub == 0, flux_before, flux_down)
                total += face_x * pltpu.roll(f, right, 1) + pltpu.roll(face_x * f, 1, 1)
                total += tz[k, at, :] * source[k + 1, at, :] + tz[k - 1, at, :] * source[k - 1, at, :]
                target[k, at, :] = 0.2 * f + we[k, at, :] * total
                f, f_up, flux_before = after, f_next, flux_down
            return carry

        lax.fori_loop(start, stop, plane, 0)

    def receive(target, start, stop):
        def one(n, carry):
            r = near[n]
            k = rec[0, 0, r] - z_first + W
            at = pl.ds(jnp.clip(rec[1, 0, r] - y_first + 8, 6, y_cells + 9), 1)

            @pl.when((k >= start) & (k < stop))
            def _():
                kc = jnp.clip(k, start, stop - 1)
                add = 2.0 * we[kc, at, :] * vals[pl.ds(r, 1), :]
                target[kc, at, :] = target[kc, at, :] + jnp.where(lane == rec[2, 0, r], add, 0.0)

            return carry

        lax.fori_loop(0, found, one, 0)

    sweep(ae, be, 1, planes - 1)

    last = (W + 1) * y_cells
    values = own[0, 7:8, :] + z_lo[last : last + 1, :] + z_hi[last : last + 1, :]
    for side in (y_lo, y_hi, lo_lo, lo_hi, hi_lo, hi_hi):
        values += side[0, 7:8, :]
    eye = lax.broadcasted_iota(jnp.int32, (count, lanes), 0) == lax.broadcasted_iota(
        jnp.int32, (count, lanes), 1
    )
    vals[...] = jnp.broadcast_to(
        jnp.sum(jnp.where(eye, values, 0.0), axis=1, keepdims=True), (count, lanes)
    )
    listing.wait()

    def listed(r, found):
        k = rec[0, 0, r] - z_first + W
        j = rec[1, 0, r] - y_first + 8
        near[found] = r
        return found + jnp.where(within(k - 1, planes - 2) & within(j - 6, y_cells + 4), 1, 0)

    found = lax.fori_loop(0, count, listed, 0, unroll=8)
    receive(be, 1, planes - 1)
    sweep(be, ae, 2, planes - 2)
    receive(ae, 2, planes - 2)


def store_kernel(ae, part, adj_out, out_sem):
    z_cells, y_cells, _ = adj_out.shape
    stores = [
        pltpu.make_async_copy(ae.at[W + k, pl.ds(8, y_cells)], adj_out.at[k], out_sem.at[k])
        for k in range(z_cells)
    ]
    for copy in stores:
        copy.start()
    for copy in stores:
        copy.wait()


def total_kernel(part, other, grad, total, sem):
    z_cells = grad.shape[0]
    stores = [pltpu.make_async_copy(total.at[k], grad.at[k], sem.at[k]) for k in range(z_cells)]
    for k in range(z_cells):
        total[k] = part[k] + other[k]
        stores[k].start()
    for copy in stores:
        copy.wait()


def gradient_kernel(pot, ae, z_lo, z_hi, y_lo, y_hi, grad, ve):
    z_cells, y_cells, lanes = pot.shape
    chunks = y_cells // 8
    sub = lax.broadcasted_iota(jnp.int32, (8, lanes), 0)
    lane = lax.broadcasted_iota(jnp.int32, (8, lanes), 1)
    right = lanes - 1
    body = pl.ds(8, y_cells)
    end = pl.ds(y_cells + 8, 8)
    plane_rows = slice(W * y_cells, (W + 1) * y_cells)
    ve[0, body, :] = z_lo[plane_rows, :]
    ve[z_cells + 1, body, :] = z_hi[plane_rows, :]
    for k in range(z_cells):
        ve[1 + k, body, :] = pot[k]
        ve[1 + k, 0:8, :], ve[1 + k, end, :] = rim_rows(sub, y_lo[k], y_hi[k], 6, 1)

    def plane(n, carry):
        k, q = n + W, n + 1

        a, v = piece(ae, k, 0, chunks), piece(ve, q, 0, chunks)
        a_after, v_after = piece(ae, k, 1, chunks), piece(ve, q, 1, chunks)
        a_up, v_up = pltpu.roll(a_after, 7, 0), pltpu.roll(v_after, 7, 0)
        term_before = pltpu.roll(
            (v - jnp.where(sub == 7, v_up, v)) * (a - jnp.where(sub == 7, a_up, a)), 1, 0
        )
        for j in range(1, chunks + 1):
            at = pl.ds(8 * j, 8)
            a, v = a_after, v_after
            a_after, v_after = piece(ae, k, j + 1, chunks), piece(ve, q, j + 1, chunks)
            a_next, v_next = pltpu.roll(a_after, 7, 0), pltpu.roll(v_after, 7, 0)
            term = (v - jnp.where(sub == 7, v_next, v_up)) * (a - jnp.where(sub == 7, a_next, a_up))
            term_down = pltpu.roll(term, 1, 0)
            total = term + jnp.where(sub == 0, term_before, term_down)
            term = (v - jnp.where(lane == right, 0.0, pltpu.roll(v, right, 1))) * (
                a - jnp.where(lane == right, 0.0, pltpu.roll(a, right, 1))
            )
            total += term + jnp.where(lane == 0, v * a, pltpu.roll(term, 1, 1))
            total += (v - ve[q - 1, at, :]) * (a - ae[k - 1, at, :])
            total += (v - ve[q + 1, at, :]) * (a - ae[k + 1, at, :])
            grad[n, pl.ds(8 * (j - 1), 8), :] = -0.5 * total
            term_before, a_up, v_up = term_down, a_next, v_next
        return carry

    lax.fori_loop(0, z_cells, plane, 0)


def shifts(devices, step):
    return [(i, i + step) for i in range(devices) if 0 <= i + step < devices]


def both_ways(up, down, axis):
    devices = lax.axis_size(axis)
    return (
        lax.ppermute(up, axis, shifts(devices, 1)), lax.ppermute(down, axis, shifts(devices, -1))
    )


def step(conductivity, receivers, observed, potential, adjoint_prev):
    cond, pot, adj = conductivity, potential[0], adjoint_prev[0]
    z_cells, y_cells, lanes = cond.shape
    count = observed.shape[1]
    shape = jax.ShapeDtypeStruct

    block = shape((z_cells, y_cells, lanes), F32)
    edge = shape((z_cells, 8, lanes), F32)
    side = shape(((W + 1) * y_cells + 8, lanes), F32)
    thick = shape((W, y_cells, lanes), F32)
    corner = shape((W, 8, lanes), F32)
    rec = receivers.transpose(1, 0, 2)
    rec, obs, cond, adj, pot = (
        pltpu.with_memory_space_constraint(x, pltpu.HBM) for x in (rec, observed, cond, adj, pot)
    )
    z_down, z_up, c_down, c_up, y_down, y_up, dd, du, ud, uu = pl.pallas_call(
        pack_kernel,
        out_shape=(side, side, thick, thick, edge, edge) + (corner,) * 4,
        in_specs=[HBM] * 5,
        out_specs=(VMEM,) * 10,
        scratch_shapes=[
            pltpu.VMEM((count, lanes), F32),
            pltpu.VMEM((z_cells, y_cells, lanes), F32),
            pltpu.VMEM((6, z_cells, 8, lanes), F32),
            pltpu.SMEM((3, 1, count), jnp.int32),
            pltpu.SMEM((1, count), F32),
            pltpu.SMEM((count,), jnp.int32),
            pltpu.SemaphoreType.DMA((6,)),
            pltpu.SemaphoreType.DMA((z_cells,)),
            pltpu.SemaphoreType.DMA((2 * W + 2,)),
            pltpu.SemaphoreType.DMA((2 * W,)),
            pltpu.SemaphoreType.DMA((2,)),
        ],
        compiler_params=pltpu.CompilerParams(vmem_limit_bytes=16 * 1024 * 1024),
        name="pack",
    )(rec, obs, cond, adj, pot)

    deep = lax.axis_size("gz")
    c_lo = lax.ppermute(c_up, ("gz", "pat"), [(2 * i + 1, 2 * i + 3) for i in range(deep - 1)])
    c_hi = lax.ppermute(c_down, ("gz", "pat"), [(2 * i + 3, 2 * i + 1) for i in range(deep - 1)])
    z_lo, z_hi = both_ways(z_up, z_down, "gz")
    y_lo, y_hi = both_ways(y_up, y_down, "gy")
    wide = lax.axis_size("gy")

    def diagonal(x, up_z, up_y):
        pairs = [
            (i * wide + j, (i + up_z) * wide + j + up_y)
            for i in range(deep) if 0 <= i + up_z < deep
            for j in range(wide) if 0 <= j + up_y < wide
        ]
        return lax.ppermute(x, ("gz", "gy"), pairs)

    lo_lo = diagonal(uu, 1, 1)
    lo_hi = diagonal(ud, 1, -1)
    hi_lo = diagonal(du, -1, 1)
    hi_hi = diagonal(dd, -1, -1)
    both = pl.pallas_call(
        join_kernel,
        out_shape=shape((2 * W, y_cells, lanes), F32),
        in_specs=[VMEM] * 2,
        out_specs=VMEM,
        compiler_params=pltpu.CompilerParams(vmem_limit_bytes=8 * 1024 * 1024),
        name="join",
    )(c_lo, c_hi)
    given = lax.ppermute(both, "pat", [(1, 0)])

    full = (z_cells + 2 * W, y_cells + 16, lanes)
    ext = shape(full, F32)
    we, tx, ty, tz = pl.pallas_call(
        weight_kernel,
        out_shape=(ext,) * 4,
        in_specs=[VMEM] * 9,
        out_specs=(VMEM,) * 4,
        scratch_shapes=[pltpu.VMEM(full, F32)],
        compiler_params=pltpu.CompilerParams(vmem_limit_bytes=20 * 1024 * 1024),
        name="weights",
    )(conductivity, both, given, y_lo, y_hi, lo_lo, lo_hi, hi_lo, hi_hi)
    relaxed = pl.pallas_call(
        sweep_kernel,
        out_shape=ext,
        in_specs=[HBM] + [VMEM] * 14,
        out_specs=VMEM,
        scratch_shapes=[
            pltpu.VMEM(full, F32),
            pltpu.VMEM((count, lanes), F32),
            pltpu.SMEM((3, 1, count), jnp.int32),
            pltpu.SMEM((count,), jnp.int32),
            pltpu.SemaphoreType.DMA,
        ],
        compiler_params=pltpu.CompilerParams(vmem_limit_bytes=20 * 1024 * 1024),
        name="sweeps",
    )(rec, adjoint_prev[0], we, tx, ty, tz, z_lo, z_hi, y_lo, y_hi, lo_lo, lo_hi, hi_lo, hi_hi, y_up)
    part = pl.pallas_call(
        gradient_kernel,
        out_shape=block,
        in_specs=[VMEM] * 6,
        out_specs=VMEM,
        scratch_shapes=[pltpu.VMEM((z_cells + 2, y_cells + 16, lanes), F32)],
        compiler_params=pltpu.CompilerParams(vmem_limit_bytes=16 * 1024 * 1024),
        name="gradient",
    )(potential[0], relaxed, z_lo, z_hi, y_lo, y_hi)
    other = lax.ppermute(part, "pat", [(0, 1), (1, 0)])
    adjoint = pl.pallas_call(
        store_kernel,
        out_shape=block,
        in_specs=[VMEM, VMEM],
        out_specs=HBM,
        scratch_shapes=[pltpu.SemaphoreType.DMA((z_cells,))],
        compiler_params=pltpu.CompilerParams(vmem_limit_bytes=4 * 1024 * 1024),
        name="store",
    )(relaxed, part)
    gradient = pl.pallas_call(
        total_kernel,
        out_shape=block,
        in_specs=[VMEM, VMEM],
        out_specs=HBM,
        scratch_shapes=[
            pltpu.VMEM((z_cells, y_cells, lanes), F32),
            pltpu.SemaphoreType.DMA((z_cells,)),
        ],
        compiler_params=pltpu.CompilerParams(vmem_limit_bytes=8 * 1024 * 1024),
        name="total",
    )(part, other)
    return adjoint[None], gradient


def solution(mesh):
    return jax.shard_map(
        step,
        mesh=mesh,
        in_specs=(
            P(("survey", "gz"), "gy", None),
            P(("survey", "pat"), None, None),
            P(("survey", "pat"), None),
            P("pat", ("survey", "gz"), "gy", None),
            P("pat", ("survey", "gz"), "gy", None),
        ),
        out_specs=(P("pat", ("survey", "gz"), "gy", None), P(("survey", "gz"), "gy", None)),
        check_vma=False,
    )
```
